32 devices in a mesh: seq: 32 (over z, y, x, core).
Axes of the slice: x: 2, y: 2, z: 4, core: 2. Of those that a mesh axis runs over, the one named last changes fastest.
Arguments:
- right_side: bfloat16 [16384, 384], P('seq'), may hold values from -6 to 6
- leaf_inverse: bfloat16 [32, 512, 512], P('seq'), may hold values from -1 to 2
- project_rows: bfloat16 [5, 16384, 128], P(None, 'seq'), may hold values from -3 to 3, as said below
- spread_rows: bfloat16 [5, 16384, 128], P(None, 'seq'), may hold values from -0.119628906 to 0.119628906
- capacity: bfloat16 [5, 4096, 256], P(None, 'seq'), may hold values from -1 to 2, as said below
Outputs:
- solution: float32 [16384, 384], P('seq')
The draws below stay inside these ranges and needn't reach their ends.
Inputs may be any that keep to these rules, and one draw needn't show every extreme that they name: Rows of project_rows of level l have a scale falling as (2 ** l * 512) ** -0.5. `capacity`: at level l the 128 x 2 * 128 blocks of all devices in one half of a node of 2 ** (l + 1) devices are equal.
All inputs are finite; a program needn't handle non-finite values.
Results may differ from the reference program's by a relative error of at most 0.0095.
Values may be sent and summed in bfloat16 or wider, within the bound.
A program may use at most 64 MiB of HBM per device.

```python
import math
import jax
import jax.numpy as jnp
from jax import lax

SEG = 512
R = 128
RHS = 384
SAMPLES = 16384
LEVELS = 5
N_SEQ = 32


def draw_leaf_inverse(key, part):
    gaussian = jnp.clip(jax.random.normal(key, (N_SEQ, SEG, SEG), jnp.float32), -4.0, 4.0)
    return (0.6 * jnp.eye(SEG, dtype=jnp.float32) + gaussian / math.sqrt(SEG)).astype(jnp.bfloat16)


def draw_project_rows(key, part):
    layers = []
    for tree_level in range(LEVELS):
        subkey = jax.random.fold_in(key, 101 + tree_level)
        gaussian = jnp.clip(jax.random.normal(subkey, (N_SEQ * SEG, R), jnp.float32), -4.0, 4.0)
        layers.append(gaussian / math.sqrt(SEG * 2 ** tree_level))
    return jnp.stack(layers).astype(jnp.bfloat16)


def draw_capacity(key, part):
    layers = []
    for tree_level in range(LEVELS):
        half_span = 2 ** tree_level
        half_count = N_SEQ // half_span
        subkey = jax.random.fold_in(key, 211 + tree_level)
        gaussian = jnp.clip(jax.random.normal(subkey, (half_count, R, 2 * R), jnp.float32), -4.0, 4.0)
        sides = jnp.arange(half_count) % 2
        column_ids = jnp.arange(2 * R)[None, None, :]
        row_ids = jnp.arange(R)[None, :, None]
        diagonal = (column_ids == row_ids + sides[:, None, None] * R).astype(jnp.float32)
        blocks = 0.6 * diagonal + 0.8 * gaussian / math.sqrt(2 * R)
        blocks = jnp.repeat(blocks, half_span, axis=0)
        layers.append(blocks.reshape(N_SEQ * R, 2 * R))
    return jnp.stack(layers).astype(jnp.bfloat16)


def levels(stream_key, extent, cuts, low, top_value):
    level = 1.0
    for position, blocks in cuts:
        steps = jax.random.uniform(jax.random.fold_in(jax.random.fold_in(stream_key, 6), position), (blocks,), jnp.float32, low / len(cuts), top_value / len(cuts))
        level = level * jnp.repeat(jnp.exp(steps), extent[position] // blocks).reshape((-1,) + (1,) * (len(extent) - 1 - position))
    return level


def normal_values(rng, shape, spread, most, cuts=(), kind=jnp.bfloat16):
    array = jax.random.normal(rng, shape, jnp.float32) * spread
    if len(cuts) > 0:
        array = levels(rng, shape, cuts, -0.22, 0.18) * array
    return jnp.clip(array, min=-most, max=most).astype(kind)


def setup_inputs(seed: int = 0) -> dict:
    keys = jax.random.split(jax.random.key(seed), 6)
    return {
        "right_side": normal_values(keys[0], (SAMPLES, RHS), 1.0, 6.0, ((0, 32),)),
        "leaf_inverse": draw_leaf_inverse(jax.random.fold_in(keys[5], 71), 0),
        "project_rows": draw_project_rows(jax.random.fold_in(keys[5], 71), 0),
        "spread_rows": normal_values(keys[3], (LEVELS, SAMPLES, R), 0.03, 0.119628906, ((1, 32),)),
        "capacity": draw_capacity(jax.random.fold_in(keys[5], 71), 0),
    }


def reference(right_side, leaf_inverse, project_rows, spread_rows, capacity):
    loaded = right_side.reshape(N_SEQ, SEG, RHS).astype(jnp.float32)
    solution = jnp.einsum("dij,djk->dik", leaf_inverse.astype(jnp.float32), loaded)
    for tree_level in range(LEVELS):
        half_span = 2 ** tree_level
        node_count = N_SEQ // (2 * half_span)
        rounded = lax.optimization_barrier(solution.astype(jnp.bfloat16)).astype(jnp.float32)
        basis_rows = project_rows[tree_level].reshape(N_SEQ, SEG, R).astype(jnp.float32)
        partial_sum = jnp.einsum("dsr,dsk->drk", basis_rows, rounded)
        node_sums = partial_sum.reshape(node_count, 2, half_span, R, RHS).sum(axis=2)
        stacked = lax.optimization_barrier(node_sums.astype(jnp.bfloat16)).astype(jnp.float32)
        stacked = stacked.reshape(node_count, 2 * R, RHS)
        node_rows = capacity[tree_level].reshape(node_count, 2, half_span, R, 2 * R)[:, :, 0].astype(jnp.float32)
        coefficients = jnp.einsum("nsrj,njk->nsrk", node_rows, stacked)
        coefficients = lax.optimization_barrier(coefficients.astype(jnp.bfloat16)).astype(jnp.float32)
        spread_all = jnp.broadcast_to(coefficients[:, :, None], (node_count, 2, half_span, R, RHS)).reshape(N_SEQ, R, RHS)
        spread_basis = spread_rows[tree_level].reshape(N_SEQ, SEG, R).astype(jnp.float32)
        solution = solution - jnp.einsum("dsr,drk->dsk", spread_basis, spread_all)
    return solution.reshape(N_SEQ * SEG, RHS)
```

```python
import functools

import jax
import jax.numpy as jnp
from jax import lax
from jax.experimental import pallas as pl
from jax.experimental.pallas import tpu as pltpu
from jax.sharding import PartitionSpec as P

MESH = pl.DeviceIdType.MESH
BF16 = jnp.bfloat16
F32 = jnp.float32


def dot_nt(left, right):
    return lax.dot_general(left, right, (((1,), (1,)), ((), ())), preferred_element_type=F32)


def dot_nn(left, right):
    return jnp.dot(left, right, preferred_element_type=F32)


def kernel(
    x_hbm, inv_hbm, p_hbm, s_hbm, c_hbm, o_hbm,
    x, inv, p, s, cap, out, p_t,
    y32, y16, y0r, z32, zs, zr, coef,
    k0s, k0r, kfull, ks, kr, g32, gs, gr,
    load_sem, send_sem, recv_sem,
):
    levels, seg, rank = p.shape
    half = y32.shape[2]
    rhs = 2 * half
    hr = rank // 2
    top = levels - 1
    me = lax.axis_index("seq")
    side = [lax.rem(lax.div(me, 1 << b), 2) for b in range(levels)]
    partner = [me + (1 - 2 * side[b]) * (1 << b) for b in range(levels)]
    core = side[0]
    pairs = [(l, m) for l in range(1, levels) for m in range(l + 1, levels)]
    first = {l: min([i for i, q in enumerate(pairs) if q[0] >= l], default=len(pairs)) for l in range(levels + 1)}
    used = [0]

    def loads(src, dst, i):
        copy = pltpu.make_async_copy(src, dst, load_sem.at[i])
        copy.start()
        return copy

    def send(src, dst, bit):
        i = used[0]
        used[0] += 1
        copy = pltpu.make_async_remote_copy(
            src_ref=src, dst_ref=dst, send_sem=send_sem.at[i], recv_sem=recv_sem.at[i],
            device_id=(partner[bit],), device_id_type=MESH,
        )
        copy.start()
        sent.append(copy)
        return copy

    sent = []
    get_p = loads(p_hbm, p, 0)
    get_s = loads(s_hbm, s, 1)
    get_c = loads(c_hbm, cap, 2)
    get_x = loads(x_hbm, x, 3)
    get_i = loads(inv_hbm.at[0], inv, 4)
    barrier = pltpu.get_barrier_semaphore()
    for b in range(levels):
        pl.semaphore_signal(barrier, inc=1, device_id=(partner[b],), device_id_type=MESH)

    get_p.wait()
    for m in range(1, levels):
        p_t[m] = p[m].T
    get_s.wait()
    get_c.wait()
    for i, (l, m) in enumerate(pairs):
        g = dot_nn(p_t[m], s[l]).reshape(2, hr, rank)
        g32[i] = g
        gs[0, i] = g.astype(BF16)
    for m in range(1, levels):
        k0s[m - 1] = dot_nn(dot_nn(p_t[m], s[0]).astype(BF16), cap[0]).astype(BF16)
    pl.semaphore_wait(barrier, levels)
    g_copy = {}
    k_copy = {}
    z_copy = {}
    c_copy = {}
    if pairs:
        g_copy[0] = send(gs.at[0, :, 1 - core], gr.at[0], 0)
    k_copy[0] = send(k0s, k0r, 0)

    get_x.wait()
    x_t = x[...].T
    get_i.wait()
    st = dot_nt(x_t, inv[...]).astype(BF16)
    for m in range(levels):
        y = dot_nn(st, p[m]).reshape(2, half, rank)
        y16[m] = y.astype(BF16)
        if m == 0:
            z_copy[0, 0] = send(y16.at[0], y0r, 0)
        else:
            y32[m] = y
    z_copy[0, 1] = send(y16.at[pl.ds(1, top), 1 - core], zr.at[0, pl.ds(1, top)], 0)

    def g_step(b):
        lo = first[b + 1]
        if lo >= len(pairs):
            return
        g_copy[b].wait_recv()
        for i in range(lo, len(pairs)):
            old = g32[i, core] if b == 0 else g32[i, 0]
            g = old + gr[b, i].astype(F32)
            g32[i, 0] = g
            if pairs[i][0] == b + 1:
                j = pairs[i][1] - (b + 2)
                kp = dot_nn(g.astype(BF16), cap[b + 1])
                ks[b + 1, j] = kp.astype(BF16)
            else:
                gs[b + 1, i, 0] = g.astype(BF16)
        n = top - (b + 1)
        k_copy[b + 1] = send(ks.at[b + 1, pl.ds(0, n)], kr.at[b + 1, pl.ds(0, n)], b + 1)
        nxt = first[b + 2]
        if nxt < len(pairs):
            rest = pl.ds(nxt, len(pairs) - nxt)
            g_copy[b + 1] = send(gs.at[b + 1, rest, 0], gr.at[b + 1, rest], b + 1)

    def k_sum(l):
        n = top - l
        k_copy[l].wait_recv()
        for j in range(n):
            kfull[l, j, core] = (ks[l, j].astype(F32) + kr[l, j].astype(F32)).astype(BF16)
        mine = kfull.at[l, pl.ds(0, n), core]
        return send(mine, mine, 0)

    def stack(own, other, l):
        low = side[l] == 0
        return jnp.concatenate([jnp.where(low, own, other), jnp.where(low, other, own)], 1)

    g_step(0)
    out[...] = dot_nn(inv[...], x[...])

    k_copy[0].wait_recv()
    for j in range(top):
        kfull[0, j] = (k0s[j].astype(F32) + k0r[j].astype(F32)).astype(BF16).reshape(2, hr, 2 * rank)
    z_copy[0, 0].wait_recv()
    stacked = stack(y16[0, core], y0r[core], 0)
    z_copy[0, 1].wait_recv()
    for m in range(1, levels):
        z = y32[m, core] + zr[0, m].astype(F32) - dot_nt(stacked, kfull[0, m - 1].reshape(rank, 2 * rank))
        z32[m] = z
        zs[1, m] = z.astype(BF16)
        z_copy[1, m] = send(zs.at[1, m], zr.at[1, m], 1)
    g_step(1)
    stacked = stack(y16[0].reshape(rhs, rank), y0r[...].reshape(rhs, rank), 0)
    coef[0] = dot_nt(stacked, cap[0]).astype(BF16).reshape(2, half, rank)
    out[...] -= dot_nt(s[0], coef[0].reshape(rhs, rank))

    for l in range(1, levels):
        if l < top:
            k_done = k_sum(l)
        z_copy[l, l].wait_recv()
        stacked = stack(zs[l, l], zr[l, l], l)
        coef[l, core] = dot_nt(stacked, cap[l]).astype(BF16)
        c_copy[l] = send(coef.at[l, core], coef.at[l, core], 0)
        if l < top:
            k_done.wait_recv()
            for m in range(l + 1, levels):
                z_copy[l, m].wait_recv()
                z = z32[m] + zr[l, m].astype(F32) - dot_nt(stacked, kfull[l, m - l - 1].reshape(rank, 2 * rank))
                z32[m] = z
                zs[l + 1, m] = z.astype(BF16)
                z_copy[l + 1, m] = send(zs.at[l + 1, m], zr.at[l + 1, m], l + 1)
            g_step(l + 1)
            c_copy[l].wait_recv()
            out[...] -= dot_nt(s[l], coef[l].reshape(rhs, rank))
    c_copy[top].wait_recv()
    c_last = coef[top].reshape(rhs, rank)
    pieces = 4
    rows = seg // pieces
    puts = []
    for i in range(pieces):
        part = pl.ds(i * rows, rows)
        out[part] = out[part] - dot_nt(s[top, part], c_last)
        puts.append(loads(out.at[part], o_hbm.at[part], 5 + i))
    for copy in sent:
        copy.wait_send()
    for put in puts:
        put.wait()


def on_device(right_side, leaf_inverse, project_rows, spread_rows, capacity):
    levels, seg, rank = project_rows.shape
    rhs = right_side.shape[1]
    half = rhs // 2
    hr = rank // 2
    pairs = max(1, (levels - 1) * (levels - 2) // 2)
    copies = levels * levels + 6 * levels
    vmem = pltpu.VMEM
    return pl.pallas_call(
        kernel,
        name="hodlr_solve",
        out_shape=jax.ShapeDtypeStruct((seg, rhs), F32),
        in_specs=[pl.BlockSpec(memory_space=pl.ANY)] * 5,
        out_specs=pl.BlockSpec(memory_space=pl.ANY),
        scratch_shapes=[
            vmem((seg, rhs), BF16),
            vmem((seg, seg), BF16),
            vmem((levels, seg, rank), BF16),
            vmem((levels, seg, rank), BF16),
            vmem((levels, rank, 2 * rank), BF16),
            vmem((seg, rhs), F32),
            vmem((levels, rank, seg), BF16),
            vmem((levels, 2, half, rank), F32),
            vmem((levels, 2, half, rank), BF16),
            vmem((2, half, rank), BF16),
            vmem((levels, half, rank), F32),
            vmem((levels, levels, half, rank), BF16),
            vmem((levels, levels, half, rank), BF16),
            vmem((levels, 2, half, rank), BF16),
            vmem((levels - 1, rank, 2 * rank), BF16),
            vmem((levels - 1, rank, 2 * rank), BF16),
            vmem((levels - 1, levels - 1, 2, hr, 2 * rank), BF16),
            vmem((levels - 1, levels - 1, hr, 2 * rank), BF16),
            vmem((levels - 1, levels - 1, hr, 2 * rank), BF16),
            vmem((pairs, 2, hr, rank), F32),
            vmem((levels - 1, pairs, 2, hr, rank), BF16),
            vmem((levels - 1, pairs, hr, rank), BF16),
            pltpu.SemaphoreType.DMA((9,)),
            pltpu.SemaphoreType.DMA((copies,)),
            pltpu.SemaphoreType.DMA((copies,)),
        ],
        compiler_params=pltpu.CompilerParams(
            collective_id=0, has_side_effects=True, vmem_limit_bytes=56 * 2**20
        ),
    )(right_side, leaf_inverse, project_rows, spread_rows, capacity)


def solution(mesh):
    return jax.shard_map(
        on_device,
        mesh=mesh,
        in_specs=(
            P("seq", None),
            P("seq", None, None),
            P(None, "seq", None),
            P(None, "seq", None),
            P(None, "seq", None),
        ),
        out_specs=P("seq", None),
        check_vma=False,
    )
```

```python
import functools

import jax
import jax.numpy as jnp
from jax import lax
from jax.experimental import pallas as pl
from jax.experimental.pallas import tpu as pltpu
from jax.sharding import PartitionSpec as P

MESH = pl.DeviceIdType.MESH
BF16 = jnp.bfloat16
F32 = jnp.float32


def dot_nt(left, right):
    return lax.dot_general(left, right, (((1,), (1,)), ((), ())), preferred_element_type=F32)


def dot_nn(left, right):
    return jnp.dot(left, right, preferred_element_type=F32)


def kernel(
    x_hbm, inv_hbm, p_hbm, s_hbm, c_hbm, out,
    x, inv, p, s, cap, p_t,
    y32, y16, y0r, z32, zs, zr, coef,
    k0s, k0r, kfull, ks, kr, g32, gs, gr,
    load_sem, send_sem, recv_sem,
):
    levels, seg, rank = p.shape
    half = y32.shape[2]
    rhs = 2 * half
    hr = rank // 2
    top = levels - 1
    me = lax.axis_index("seq")
    side = [lax.rem(lax.div(me, 1 << b), 2) for b in range(levels)]
    partner = [me + (1 - 2 * side[b]) * (1 << b) for b in range(levels)]
    core = side[0]
    pairs = [(l, m) for l in range(1, levels) for m in range(l + 1, levels)]
    first = {l: min([i for i, q in enumerate(pairs) if q[0] >= l], default=len(pairs)) for l in range(levels + 1)}
    used = [0]

    def loads(src, dst, i):
        copy = pltpu.make_async_copy(src, dst, load_sem.at[i])
        copy.start()
        return copy

    def send(src, dst, bit):
        i = used[0]
        used[0] += 1
        copy = pltpu.make_async_remote_copy(
            src_ref=src, dst_ref=dst, send_sem=send_sem.at[i], recv_sem=recv_sem.at[i],
            device_id=(partner[bit],), device_id_type=MESH,
        )
        copy.start()
        sent.append(copy)
        return copy

    sent = []
    get_p = loads(p_hbm, p, 0)
    get_s = loads(s_hbm, s, 1)
    get_c = loads(c_hbm, cap, 2)
    get_x = loads(x_hbm, x, 3)
    get_i = loads(inv_hbm.at[0], inv, 4)
    barrier = pltpu.get_barrier_semaphore()
    for b in range(levels):
        pl.semaphore_signal(barrier, inc=1, device_id=(partner[b],), device_id_type=MESH)

    get_p.wait()
    for m in range(1, levels):
        p_t[m] = p[m].T
    get_s.wait()
    get_c.wait()
    for i, (l, m) in enumerate(pairs):
        g = dot_nn(p_t[m], s[l]).reshape(2, hr, rank)
        g32[i] = g
        gs[0, i] = g.astype(BF16)
    for m in range(1, levels):
        k0s[m - 1] = dot_nn(dot_nn(p_t[m], s[0]).astype(BF16), cap[0]).astype(BF16)
    pl.semaphore_wait(barrier, levels)
    g_copy = {}
    k_copy = {}
    z_copy = {}
    c_copy = {}
    if pairs:
        g_copy[0] = send(gs.at[0, :, 1 - core], gr.at[0], 0)
    k_copy[0] = send(k0s, k0r, 0)

    get_x.wait()
    x_t = x[...].T
    get_i.wait()
    st = dot_nt(x_t, inv[...]).astype(BF16)
    for m in range(levels):
        y = dot_nn(st, p[m]).reshape(2, half, rank)
        y16[m] = y.astype(BF16)
        if m == 0:
            z_copy[0, 0] = send(y16.at[0], y0r, 0)
        else:
            y32[m] = y
    z_copy[0, 1] = send(y16.at[pl.ds(1, top), 1 - core], zr.at[0, pl.ds(1, top)], 0)

    def g_step(b):
        lo = first[b + 1]
        if lo >= len(pairs):
            return
        g_copy[b].wait_recv()
        for i in range(lo, len(pairs)):
            old = g32[i, core] if b == 0 else g32[i, 0]
            g = old + gr[b, i].astype(F32)
            g32[i, 0] = g
            if pairs[i][0] == b + 1:
                j = pairs[i][1] - (b + 2)
                kp = dot_nn(g.astype(BF16), cap[b + 1])
                ks[b + 1, j] = kp.astype(BF16)
            else:
                gs[b + 1, i, 0] = g.astype(BF16)
        n = top - (b + 1)
        k_copy[b + 1] = send(ks.at[b + 1, pl.ds(0, n)], kr.at[b + 1, pl.ds(0, n)], b + 1)
        nxt = first[b + 2]
        if nxt < len(pairs):
            rest = pl.ds(nxt, len(pairs) - nxt)
            g_copy[b + 1] = send(gs.at[b + 1, rest, 0], gr.at[b + 1, rest], b + 1)

    def k_sum(l):
        n = top - l
        k_copy[l].wait_recv()
        for j in range(n):
            kfull[l, j, core] = (ks[l, j].astype(F32) + kr[l, j].astype(F32)).astype(BF16)
        mine = kfull.at[l, pl.ds(0, n), core]
        return send(mine, mine, 0)

    def stack(own, other, l):
        low = side[l] == 0
        return jnp.concatenate([jnp.where(low, own, other), jnp.where(low, other, own)], 1)

    g_step(0)
    out[...] = dot_nn(inv[...], x[...])

    k_copy[0].wait_recv()
    for j in range(top):
        kfull[0, j] = (k0s[j].astype(F32) + k0r[j].astype(F32)).astype(BF16).reshape(2, hr, 2 * rank)
    z_copy[0, 0].wait_recv()
    stacked = stack(y16[0, core], y0r[core], 0)
    z_copy[0, 1].wait_recv()
    for m in range(1, levels):
        z = y32[m, core] + zr[0, m].astype(F32) - dot_nt(stacked, kfull[0, m - 1].reshape(rank, 2 * rank))
        z32[m] = z
        zs[1, m] = z.astype(BF16)
        z_copy[1, m] = send(zs.at[1, m], zr.at[1, m], 1)
    g_step(1)
    stacked = stack(y16[0].reshape(rhs, rank), y0r[...].reshape(rhs, rank), 0)
    coef[0] = dot_nt(stacked, cap[0]).astype(BF16).reshape(2, half, rank)
    out[...] -= dot_nt(s[0], coef[0].reshape(rhs, rank))

    for l in range(1, levels):
        if l < top:
            k_done = k_sum(l)
        z_copy[l, l].wait_recv()
        stacked = stack(zs[l, l], zr[l, l], l)
        coef[l, core] = dot_nt(stacked, cap[l]).astype(BF16)
        c_copy[l] = send(coef.at[l, core], coef.at[l, core], 0)
        if l < top:
            k_done.wait_recv()
            for m in range(l + 1, levels):
                z_copy[l, m].wait_recv()
                z = z32[m] + zr[l, m].astype(F32) - dot_nt(stacked, kfull[l, m - l - 1].reshape(rank, 2 * rank))
                z32[m] = z
                zs[l + 1, m] = z.astype(BF16)
                z_copy[l + 1, m] = send(zs.at[l + 1, m], zr.at[l + 1, m], l + 1)
            g_step(l + 1)
            c_copy[l].wait_recv()
            out[...] -= dot_nt(s[l], coef[l].reshape(rhs, rank))
    c_copy[top].wait_recv()
    c_last = coef[top].reshape(rhs, rank)
    out[...] -= dot_nt(s[top], c_last)
    for copy in sent:
        copy.wait_send()


def on_device(right_side, leaf_inverse, project_rows, spread_rows, capacity):
    levels, seg, rank = project_rows.shape
    rhs = right_side.shape[1]
    half = rhs // 2
    hr = rank // 2
    pairs = max(1, (levels - 1) * (levels - 2) // 2)
    copies = levels * levels + 6 * levels
    vmem = pltpu.VMEM
    return pl.pallas_call(
        kernel,
        name="hodlr_solve",
        out_shape=pltpu.VMEM((seg, rhs), F32),
        in_specs=[pl.BlockSpec(memory_space=pltpu.HBM)] * 5,
        out_specs=pl.BlockSpec(memory_space=pltpu.VMEM),
        scratch_shapes=[
            vmem((seg, rhs), BF16),
            vmem((seg, seg), BF16),
            vmem((levels, seg, rank), BF16),
            vmem((levels, seg, rank), BF16),
            vmem((levels, rank, 2 * rank), BF16),
            vmem((levels, rank, seg), BF16),
            vmem((levels, 2, half, rank), F32),
            vmem((levels, 2, half, rank), BF16),
            vmem((2, half, rank), BF16),
            vmem((levels, half, rank), F32),
            vmem((levels, levels, half, rank), BF16),
            vmem((levels, levels, half, rank), BF16),
            vmem((levels, 2, half, rank), BF16),
            vmem((levels - 1, rank, 2 * rank), BF16),
            vmem((levels - 1, rank, 2 * rank), BF16),
            vmem((levels - 1, levels - 1, 2, hr, 2 * rank), BF16),
            vmem((levels - 1, levels - 1, hr, 2 * rank), BF16),
            vmem((levels - 1, levels - 1, hr, 2 * rank), BF16),
            vmem((pairs, 2, hr, rank), F32),
            vmem((levels - 1, pairs, 2, hr, rank), BF16),
            vmem((levels - 1, pairs, hr, rank), BF16),
            pltpu.SemaphoreType.DMA((5,)),
            pltpu.SemaphoreType.DMA((copies,)),
            pltpu.SemaphoreType.DMA((copies,)),
        ],
        compiler_params=pltpu.CompilerParams(
            collective_id=0, has_side_effects=True, vmem_limit_bytes=56 * 2**20
        ),
    )(right_side, leaf_inverse, project_rows, spread_rows, capacity)


def solution(mesh):
    return jax.shard_map(
        on_device,
        mesh=mesh,
        in_specs=(
            P("seq", None),
            P("seq", None, None),
            P(None, "seq", None),
            P(None, "seq", None),
            P(None, "seq", None),
        ),
        out_specs=P("seq", None),
        check_vma=False,
    )
```

```python
import functools

import jax
import jax.numpy as jnp
from jax import lax
from jax.experimental import pallas as pl
from jax.experimental.pallas import tpu as pltpu
from jax.sharding import PartitionSpec as P

MESH = pl.DeviceIdType.MESH
BF16 = jnp.bfloat16
F32 = jnp.float32


def dot_nt(left, right):
    return lax.dot_general(left, right, (((1,), (1,)), ((), ())), preferred_element_type=F32)


def dot_nn(left, right):
    return jnp.dot(left, right, preferred_element_type=F32)


def kernel(
    x_hbm, inv_hbm, p_hbm, s_hbm, c_hbm, out,
    x, inv, p, s, cap, p_t,
    y32, y16, y0r, zr0, z1s, z1r, zb32, zb16, zbr, z32, zs, zr, coef,
    g1f, g1s, g1r, k0s, k0r, kfull, ks, kr, g32, gs, gr,
    load_sem, send_sem, recv_sem,
):
    levels, seg, rank = p.shape
    half = y32.shape[2]
    quarter = half // 2
    rhs = 2 * half
    hr = rank // 2
    top = levels - 1
    me = lax.axis_index("seq")
    side = [lax.rem(lax.div(me, 1 << b), 2) for b in range(levels)]
    partner = [me + (1 - 2 * side[b]) * (1 << b) for b in range(levels)]
    core = side[0]
    xside = side[1]
    diagonal = partner[1] + partner[0] - me
    pairs = [(l, m) for l in range(2, levels) for m in range(l + 1, levels)]
    first = {l: min([i for i, q in enumerate(pairs) if q[0] >= l], default=len(pairs)) for l in range(levels + 1)}
    used = [0]

    def loads(src, dst, i):
        copy = pltpu.make_async_copy(src, dst, load_sem.at[i])
        copy.start()
        return copy

    def send(src, dst, bit, target=None):
        i = used[0]
        used[0] += 1
        copy = pltpu.make_async_remote_copy(
            src_ref=src, dst_ref=dst, send_sem=send_sem.at[i], recv_sem=recv_sem.at[i],
            device_id=(partner[bit] if target is None else target,), device_id_type=MESH,
        )
        copy.start()
        sent.append(copy)
        return copy

    sent = []
    get_p = loads(p_hbm, p, 0)
    get_s = loads(s_hbm, s, 1)
    get_c = loads(c_hbm, cap, 2)
    get_x = loads(x_hbm, x, 3)
    get_i = loads(inv_hbm.at[0], inv, 4)
    barrier = pltpu.get_barrier_semaphore()
    for b in range(levels):
        pl.semaphore_signal(barrier, inc=1, device_id=(partner[b],), device_id_type=MESH)
    pl.semaphore_signal(barrier, inc=1, device_id=(diagonal,), device_id_type=MESH)

    get_p.wait()
    for m in range(1, levels):
        p_t[m] = p[m].T
    get_s.wait()
    get_c.wait()
    for l in range(1, levels - 1):
        products = dot_nn(p_t[l + 1 : levels].reshape((top - l) * rank, seg), s[l])
        if l == 1:
            g1f[...] = products
            g1s[...] = products.astype(BF16)
        else:
            products = products.reshape(top - l, 2, hr, rank)
            g32[first[l] : first[l] + top - l] = products
            gs[0, first[l] : first[l] + top - l] = products.astype(BF16)
    products = dot_nn(p_t[1:levels].reshape(top * rank, seg), s[0]).astype(BF16)
    k0s[...] = dot_nn(products, cap[0]).astype(BF16)
    pl.semaphore_wait(barrier, levels + 1)
    g_copy = {}
    k_copy = {}
    z_copy = {}
    c_copy = {}
    if pairs:
        g_copy[0] = send(gs.at[0, :, 1 - core], gr.at[0], 0)
    g1_copy = send(g1s, g1r, 0)
    k_copy[0] = send(k0s, k0r, 0)

    get_x.wait()
    x_t = x[...].T
    get_i.wait()
    st = dot_nt(x_t, inv[...]).astype(BF16)
    for m in range(levels):
        y = dot_nn(st, p[m]).reshape(2, half, rank)
        y16[m] = y.astype(BF16)
        if m == 0:
            z_copy[0, 0] = send(y16.at[0], y0r, 0)
        else:
            y32[m] = y
    z_copy[0, 1] = send(y16.at[pl.ds(1, top), 1 - core], zr0.at[pl.ds(1, top)], 0)

    def g_step(b):
        lo = first[b + 1]
        if lo >= len(pairs):
            return
        g_copy[b].wait_recv()
        for i in range(lo, len(pairs)):
            old = g32[i, core] if b == 0 else g32[i, 0]
            g = old + gr[b, i].astype(F32)
            g32[i, 0] = g
            if pairs[i][0] == b + 1:
                j = pairs[i][1] - (b + 2)
                kp = dot_nn(g.astype(BF16), cap[b + 1])
                ks[b + 1, j] = kp.astype(BF16)
            else:
                gs[b + 1, i, 0] = g.astype(BF16)
        if b >= 1:
            n = top - (b + 1)
            k_copy[b + 1] = send(ks.at[b + 1, pl.ds(0, n)], kr.at[b + 1, pl.ds(0, n)], b + 1)
        nxt = first[b + 2]
        if nxt < len(pairs):
            rest = pl.ds(nxt, len(pairs) - nxt)
            g_copy[b + 1] = send(gs.at[b + 1, rest, 0], gr.at[b + 1, rest], b + 1)

    def k_sum(l):
        n = top - l
        k_copy[l].wait_recv()
        for j in range(n):
            kfull[l, j, core] = (ks[l, j].astype(F32) + kr[l, j].astype(F32)).astype(BF16)
        mine = kfull.at[l, pl.ds(0, n), core]
        return send(mine, mine, 0)

    def stack(own, other, l):
        low = side[l] == 0
        return jnp.concatenate([jnp.where(low, own, other), jnp.where(low, other, own)], 1)

    g_step(0)

    k_copy[0].wait_recv()
    k0r[...] = (k0s[...].astype(F32) + k0r[...].astype(F32)).astype(BF16)
    z_copy[0, 0].wait_recv()
    stacked = stack(y16[0, core], y0r[core], 0)
    z_copy[0, 1].wait_recv()
    for m in range(1, levels):
        z = y32[m, core] + zr0[m].astype(F32) - dot_nt(stacked, k0r[(m - 1) * rank : m * rank])
        if m == 1:
            z1s[...] = z.astype(BF16)
            z_copy[1, 1] = send(z1s, z1r, 1)
        else:
            zb32[m] = z.reshape(2, quarter, rank)
    g1_copy.wait_recv()
    g1s_sum = (g1f[...] + g1r[...].astype(F32)).astype(BF16)
    g1f[...] = g1s_sum.astype(F32)
    g_step(1)
    out[...] = dot_nn(inv[...], x[...])
    stacked = stack(y16[0].reshape(rhs, rank), y0r[...].reshape(rhs, rank), 0)
    coef[0] = dot_nt(stacked, cap[0]).astype(BF16).reshape(2, 2, quarter, rank)
    out[...] -= dot_nt(s[0], coef[0].reshape(rhs, rank))

    z_copy[1, 1].wait_recv()
    c_one = dot_nt(stack(z1s[...], z1r[...], 1), cap[1]).astype(BF16)
    coef[1, core] = c_one.reshape(2, quarter, rank)
    for m in range(2, levels):
        g = g1f[(m - 2) * rank : (m - 1) * rank].astype(BF16)
        z = zb32[m] - dot_nt(c_one, g).reshape(2, quarter, rank)
        zb32[m] = z
        zb16[m] = z.astype(BF16)
        z_copy[1, m] = send(zb16.at[m, 1 - xside], zbr.at[m], 1)
    c_copy[1] = send(coef.at[1, core], coef.at[1, core], 0)
    k_done = k_sum(2)
    c_copy[1].wait_recv()
    out[...] -= dot_nt(s[1], coef[1].reshape(rhs, rank))
    for m in range(2, levels):
        z_copy[1, m].wait_recv()
        z = zb32[m, xside] + zbr[m].astype(F32)
        z32[m] = z
        zs[2, m] = z.astype(BF16)
        z_copy[2, m] = send(zs.at[2, m], zr.at[2, m], 2)
    g_step(2)

    for l in range(2, levels):
        z_copy[l, l].wait_recv()
        stacked = stack(zs[l, l], zr[l, l], l)
        if l < top:
            k_done.wait_recv()
            for m in range(l + 1, levels):
                z_copy[l, m].wait_recv()
                z = z32[m] + zr[l, m].astype(F32) - dot_nt(stacked, kfull[l, m - l - 1].reshape(rank, 2 * rank))
                z32[m] = z
                zs[l + 1, m] = z.astype(BF16)
                z_copy[l + 1, m] = send(zs.at[l + 1, m], zr.at[l + 1, m], l + 1)
        coef[l, core, xside] = dot_nt(stacked, cap[l]).astype(BF16)
        mine = coef.at[l, core, xside]
        c_copy[l] = [send(mine, mine, 1, diagonal), send(mine, mine, 1), send(mine, mine, 0)]
        if l < top:
            if l + 1 < top:
                g_step(l + 1)
                k_done = k_sum(l + 1)
            for copy in c_copy[l]:
                copy.wait_recv()
            out[...] -= dot_nt(s[l], coef[l].reshape(rhs, rank))
    for copy in c_copy[top]:
        copy.wait_recv()
    c_last = coef[top].reshape(rhs, rank)
    out[...] -= dot_nt(s[top], c_last)
    for copy in sent:
        copy.wait_send()


def on_device(right_side, leaf_inverse, project_rows, spread_rows, capacity):
    levels, seg, rank = project_rows.shape
    rhs = right_side.shape[1]
    half = rhs // 2
    quarter = half // 2
    hr = rank // 2
    pairs = max(1, (levels - 2) * (levels - 3) // 2)
    copies = levels * levels + 6 * levels
    vmem = pltpu.VMEM
    return pl.pallas_call(
        kernel,
        name="hodlr_solve",
        out_shape=pltpu.VMEM((seg, rhs), F32),
        in_specs=[pl.BlockSpec(memory_space=pltpu.HBM)] * 5,
        out_specs=pl.BlockSpec(memory_space=pltpu.VMEM),
        scratch_shapes=[
            vmem((seg, rhs), BF16),
            vmem((seg, seg), BF16),
            vmem((levels, seg, rank), BF16),
            vmem((levels, seg, rank), BF16),
            vmem((levels, rank, 2 * rank), BF16),
            vmem((levels, rank, seg), BF16),
            vmem((levels, 2, half, rank), F32),
            vmem((levels, 2, half, rank), BF16),
            vmem((2, half, rank), BF16),
            vmem((levels, half, rank), BF16),
            vmem((half, rank), BF16),
            vmem((half, rank), BF16),
            vmem((levels, 2, quarter, rank), F32),
            vmem((levels, 2, quarter, rank), BF16),
            vmem((levels, quarter, rank), BF16),
            vmem((levels, quarter, rank), F32),
            vmem((levels, levels, quarter, rank), BF16),
            vmem((levels, levels, quarter, rank), BF16),
            vmem((levels, 2, 2, quarter, rank), BF16),
            vmem(((levels - 2) * rank, rank), F32),
            vmem(((levels - 2) * rank, rank), BF16),
            vmem(((levels - 2) * rank, rank), BF16),
            vmem(((levels - 1) * rank, 2 * rank), BF16),
            vmem(((levels - 1) * rank, 2 * rank), BF16),
            vmem((levels - 1, levels - 1, 2, hr, 2 * rank), BF16),
            vmem((levels - 1, levels - 1, hr, 2 * rank), BF16),
            vmem((levels - 1, levels - 1, hr, 2 * rank), BF16),
            vmem((pairs, 2, hr, rank), F32),
            vmem((levels - 1, pairs, 2, hr, rank), BF16),
            vmem((levels - 1, pairs, hr, rank), BF16),
            pltpu.SemaphoreType.DMA((5,)),
            pltpu.SemaphoreType.DMA((copies,)),
            pltpu.SemaphoreType.DMA((copies,)),
        ],
        compiler_params=pltpu.CompilerParams(
            collective_id=0, has_side_effects=True, vmem_limit_bytes=56 * 2**20
        ),
    )(right_side, leaf_inverse, project_rows, spread_rows, capacity)


def solution(mesh):
    return jax.shard_map(
        on_device,
        mesh=mesh,
        in_specs=(
            P("seq", None),
            P("seq", None, None),
            P(None, "seq", None),
            P(None, "seq", None),
            P(None, "seq", None),
        ),
        out_specs=P("seq", None),
        check_vma=False,
    )
```

```python
import functools

import jax
import jax.numpy as jnp
from jax import lax
from jax.experimental import pallas as pl
from jax.experimental.pallas import tpu as pltpu
from jax.sharding import PartitionSpec as P

MESH = pl.DeviceIdType.MESH
BF16 = jnp.bfloat16
F32 = jnp.float32


def dot_nt(left, right):
    return lax.dot_general(left, right, (((1,), (1,)), ((), ())), preferred_element_type=F32)


def dot_nn(left, right):
    return jnp.dot(left, right, preferred_element_type=F32)


def kernel(
    x_hbm, inv_hbm, p_hbm, s_hbm, c_hbm, out,
    x, inv, p, s, cap, p_t,
    y32, y16, y0r, zr0, z1s, z1r, zb32, zb16, zbr, z32, zs, zr, coef,
    g1f, g1s, g1r, k0s, k0r, kfull, ks, kr, g32, gs, gr,
    load_sem, send_sem, recv_sem,
):
    levels, seg, rank = p.shape
    half = y32.shape[2]
    quarter = half // 2
    rhs = 2 * half
    hr = rank // 2
    top = levels - 1
    me = lax.axis_index("seq")
    side = [lax.rem(lax.div(me, 1 << b), 2) for b in range(levels)]
    partner = [me + (1 - 2 * side[b]) * (1 << b) for b in range(levels)]
    core = side[0]
    xside = side[1]
    diagonal = partner[1] + partner[0] - me
    pairs = [(l, m) for l in range(2, levels) for m in range(l + 1, levels)]
    first = {l: min([i for i, q in enumerate(pairs) if q[0] >= l], default=len(pairs)) for l in range(levels + 1)}
    used = [0]

    def loads(src, dst, i):
        copy = pltpu.make_async_copy(src, dst, load_sem.at[i])
        copy.start()
        return copy

    def send(src, dst, bit, target=None):
        i = used[0]
        used[0] += 1
        copy = pltpu.make_async_remote_copy(
            src_ref=src, dst_ref=dst, send_sem=send_sem.at[i], recv_sem=recv_sem.at[i],
            device_id=(partner[bit] if target is None else target,), device_id_type=MESH,
        )
        copy.start()
        sent.append(copy)
        return copy

    sent = []
    get_x = loads(x_hbm, x, 0)
    get_i = loads(inv_hbm.at[0], inv, 1)
    get_p = loads(p_hbm, p, 2)
    get_s = loads(s_hbm, s, 3)
    get_c = loads(c_hbm, cap, 4)
    barrier = pltpu.get_barrier_semaphore()
    for b in range(levels):
        pl.semaphore_signal(barrier, inc=1, device_id=(partner[b],), device_id_type=MESH)
    pl.semaphore_signal(barrier, inc=1, device_id=(diagonal,), device_id_type=MESH)

    g_copy = {}
    k_copy = {}
    z_copy = {}
    c_copy = {}

    get_x.wait()
    x_t = x[...].T
    get_i.wait()
    st = dot_nt(x_t, inv[...]).astype(BF16)
    get_p.wait()
    for m in range(levels):
        y = dot_nn(st, p[m]).reshape(2, half, rank)
        y16[m] = y.astype(BF16)
        if m > 0:
            y32[m] = y
    pl.semaphore_wait(barrier, levels + 1)
    z_copy[0, 0] = send(y16.at[0], y0r, 0)
    z_copy[0, 1] = send(y16.at[pl.ds(1, top), 1 - core], zr0.at[pl.ds(1, top)], 0)

    for m in range(1, levels):
        p_t[m] = p[m].T
    get_s.wait()
    get_c.wait()
    products = dot_nn(p_t[1:levels].reshape(top * rank, seg), s[0]).astype(BF16)
    k0s[...] = dot_nn(products, cap[0]).astype(BF16)
    k_copy[0] = send(k0s, k0r, 0)
    for l in range(levels - 2, 0, -1):
        products = dot_nn(p_t[l + 1 : levels].reshape((top - l) * rank, seg), s[l])
        if l == 1:
            g1f[...] = products
            g1s[...] = products.astype(BF16)
            g1_copy = send(g1s, g1r, 0)
        else:
            products = products.reshape(top - l, 2, hr, rank)
            g32[first[l] : first[l] + top - l] = products
            gs[0, first[l] : first[l] + top - l] = products.astype(BF16)
            if l == 2:
                g_copy[0] = send(gs.at[0, :, 1 - core], gr.at[0], 0)

    def g_step(b):
        lo = first[b + 1]
        if lo >= len(pairs):
            return
        g_copy[b].wait_recv()
        for i in range(lo, len(pairs)):
            old = g32[i, core] if b == 0 else g32[i, 0]
            g = old + gr[b, i].astype(F32)
            g32[i, 0] = g
            if pairs[i][0] == b + 1:
                j = pairs[i][1] - (b + 2)
                kp = dot_nn(g.astype(BF16), cap[b + 1])
                ks[b + 1, j] = kp.astype(BF16)
            else:
                gs[b + 1, i, 0] = g.astype(BF16)
        if b >= 1:
            n = top - (b + 1)
            k_copy[b + 1] = send(ks.at[b + 1, pl.ds(0, n)], kr.at[b + 1, pl.ds(0, n)], b + 1)
        nxt = first[b + 2]
        if nxt < len(pairs):
            rest = pl.ds(nxt, len(pairs) - nxt)
            g_copy[b + 1] = send(gs.at[b + 1, rest, 0], gr.at[b + 1, rest], b + 1)

    def k_sum(l):
        n = top - l
        k_copy[l].wait_recv()
        for j in range(n):
            kfull[l, j, core] = (ks[l, j].astype(F32) + kr[l, j].astype(F32)).astype(BF16)
        mine = kfull.at[l, pl.ds(0, n), core]
        return send(mine, mine, 0)

    def stack(own, other, l):
        low = side[l] == 0
        return jnp.concatenate([jnp.where(low, own, other), jnp.where(low, other, own)], 1)

    k_copy[0].wait_recv()
    k0r[...] = (k0s[...].astype(F32) + k0r[...].astype(F32)).astype(BF16)
    z_copy[0, 0].wait_recv()
    stacked = stack(y16[0, core], y0r[core], 0)
    z_copy[0, 1].wait_recv()
    for m in range(1, levels):
        z = y32[m, core] + zr0[m].astype(F32) - dot_nt(stacked, k0r[(m - 1) * rank : m * rank])
        if m == 1:
            z1s[...] = z.astype(BF16)
            z_copy[1, 1] = send(z1s, z1r, 1)
        else:
            zb32[m] = z.reshape(2, quarter, rank)
    g_step(0)
    g1_copy.wait_recv()
    g1s_sum = (g1f[...] + g1r[...].astype(F32)).astype(BF16)
    g1f[...] = g1s_sum.astype(F32)
    out[...] = dot_nn(inv[...], x[...])
    stacked = stack(y16[0].reshape(rhs, rank), y0r[...].reshape(rhs, rank), 0)
    coef[0] = dot_nt(stacked, cap[0]).astype(BF16).reshape(2, 2, quarter, rank)
    out[...] -= dot_nt(s[0], coef[0].reshape(rhs, rank))

    z_copy[1, 1].wait_recv()
    c_one = dot_nt(stack(z1s[...], z1r[...], 1), cap[1]).astype(BF16)
    coef[1, core] = c_one.reshape(2, quarter, rank)
    for m in range(2, levels):
        g = g1f[(m - 2) * rank : (m - 1) * rank].astype(BF16)
        z = zb32[m] - dot_nt(c_one, g).reshape(2, quarter, rank)
        zb32[m] = z
        zb16[m] = z.astype(BF16)
        z_copy[1, m] = send(zb16.at[m, 1 - xside], zbr.at[m], 1)
    c_copy[1] = send(coef.at[1, core], coef.at[1, core], 0)
    g_step(1)
    for m in range(2, levels):
        z_copy[1, m].wait_recv()
        z = zb32[m, xside] + zbr[m].astype(F32)
        z32[m] = z
        zs[2, m] = z.astype(BF16)
        z_copy[2, m] = send(zs.at[2, m], zr.at[2, m], 2)
    k_done = k_sum(2)
    g_step(2)
    c_copy[1].wait_recv()
    out[...] -= dot_nt(s[1], coef[1].reshape(rhs, rank))

    for l in range(2, levels):
        z_copy[l, l].wait_recv()
        stacked = stack(zs[l, l], zr[l, l], l)
        if l < top:
            k_done.wait_recv()
            for m in range(l + 1, levels):
                z_copy[l, m].wait_recv()
                z = z32[m] + zr[l, m].astype(F32) - dot_nt(stacked, kfull[l, m - l - 1].reshape(rank, 2 * rank))
                z32[m] = z
                zs[l + 1, m] = z.astype(BF16)
                z_copy[l + 1, m] = send(zs.at[l + 1, m], zr.at[l + 1, m], l + 1)
        coef[l, core, xside] = dot_nt(stacked, cap[l]).astype(BF16)
        mine = coef.at[l, core, xside]
        c_copy[l] = [send(mine, mine, 1, diagonal), send(mine, mine, 1), send(mine, mine, 0)]
        if l < top:
            if l + 1 < top:
                k_done = k_sum(l + 1)
                g_step(l + 1)
    for l in range(2, levels):
        for copy in c_copy[l]:
            copy.wait_recv()
        if l < top:
            out[...] -= dot_nt(s[l], coef[l].reshape(rhs, rank))
    for copy in sent:
        copy.wait_send()
    c_last = coef[top].reshape(rhs, rank)
    out[...] -= dot_nt(s[top], c_last)


def on_device(right_side, leaf_inverse, project_rows, spread_rows, capacity):
    levels, seg, rank = project_rows.shape
    rhs = right_side.shape[1]
    half = rhs // 2
    quarter = half // 2
    hr = rank // 2
    pairs = max(1, (levels - 2) * (levels - 3) // 2)
    copies = levels * levels + 6 * levels
    vmem = pltpu.VMEM
    return pl.pallas_call(
        kernel,
        name="hodlr_solve",
        out_shape=pltpu.VMEM((seg, rhs), F32),
        in_specs=[pl.BlockSpec(memory_space=pltpu.HBM)] * 5,
        out_specs=pl.BlockSpec(memory_space=pltpu.VMEM),
        scratch_shapes=[
            vmem((seg, rhs), BF16),
            vmem((seg, seg), BF16),
            vmem((levels, seg, rank), BF16),
            vmem((levels, seg, rank), BF16),
            vmem((levels, rank, 2 * rank), BF16),
            vmem((levels, rank, seg), BF16),
            vmem((levels, 2, half, rank), F32),
            vmem((levels, 2, half, rank), BF16),
            vmem((2, half, rank), BF16),
            vmem((levels, half, rank), BF16),
            vmem((half, rank), BF16),
            vmem((half, rank), BF16),
            vmem((levels, 2, quarter, rank), F32),
            vmem((levels, 2, quarter, rank), BF16),
            vmem((levels, quarter, rank), BF16),
            vmem((levels, quarter, rank), F32),
            vmem((levels, levels, quarter, rank), BF16),
            vmem((levels, levels, quarter, rank), BF16),
            vmem((levels, 2, 2, quarter, rank), BF16),
            vmem(((levels - 2) * rank, rank), F32),
            vmem(((levels - 2) * rank, rank), BF16),
            vmem(((levels - 2) * rank, rank), BF16),
            vmem(((levels - 1) * rank, 2 * rank), BF16),
            vmem(((levels - 1) * rank, 2 * rank), BF16),
            vmem((levels - 1, levels - 1, 2, hr, 2 * rank), BF16),
            vmem((levels - 1, levels - 1, hr, 2 * rank), BF16),
            vmem((levels - 1, levels - 1, hr, 2 * rank), BF16),
            vmem((pairs, 2, hr, rank), F32),
            vmem((levels - 1, pairs, 2, hr, rank), BF16),
            vmem((levels - 1, pairs, hr, rank), BF16),
            pltpu.SemaphoreType.DMA((5,)),
            pltpu.SemaphoreType.DMA((copies,)),
            pltpu.SemaphoreType.DMA((copies,)),
        ],
        compiler_params=pltpu.CompilerParams(
            collective_id=0, has_side_effects=True, vmem_limit_bytes=56 * 2**20
        ),
    )(right_side, leaf_inverse, project_rows, spread_rows, capacity)


def solution(mesh):
    return jax.shard_map(
        on_device,
        mesh=mesh,
        in_specs=(
            P("seq", None),
            P("seq", None, None),
            P(None, "seq", None),
            P(None, "seq", None),
            P(None, "seq", None),
        ),
        out_specs=P("seq", None),
        check_vma=False,
    )
```

```python
import functools

import jax
import jax.numpy as jnp
from jax import lax
from jax.experimental import pallas as pl
from jax.experimental.pallas import tpu as pltpu
from jax.sharding import PartitionSpec as P

MESH = pl.DeviceIdType.MESH
BF16 = jnp.bfloat16
F32 = jnp.float32


def dot_nt(left, right):
    return lax.dot_general(left, right, (((1,), (1,)), ((), ())), preferred_element_type=F32)


def dot_nn(left, right):
    return jnp.dot(left, right, preferred_element_type=F32)


def kernel(
    x_hbm, inv_hbm, p_hbm, s_hbm, c_hbm, out,
    x, inv, p, s, cap, p_t,
    y32, y16, y0r, zr0, z1s, z1r, zb32, zb16, zbr, z32, zs, zr, coef,
    g1f, g1s, g1r, k0s, k0r, kfull, ks, kr, g32, gs, gr,
    load_sem, send_sem, recv_sem,
):
    levels, seg, rank = p.shape
    half = y32.shape[2]
    quarter = half // 2
    rhs = 2 * half
    hr = rank // 2
    top = levels - 1
    me = lax.axis_index("seq")
    side = [lax.rem(lax.div(me, 1 << b), 2) for b in range(levels)]
    partner = [me + (1 - 2 * side[b]) * (1 << b) for b in range(levels)]
    core = side[0]
    xside = side[1]
    diagonal = partner[1] + partner[0] - me
    pairs = [(l, m) for l in range(2, levels) for m in range(l + 1, levels)]
    first = {l: min([i for i, q in enumerate(pairs) if q[0] >= l], default=len(pairs)) for l in range(levels + 1)}
    used = [0]

    def loads(src, dst, i):
        copy = pltpu.make_async_copy(src, dst, load_sem.at[i])
        copy.start()
        return copy

    def send(src, dst, bit, target=None):
        i = used[0]
        used[0] += 1
        out_i = free.pop(0)
        copy = pltpu.make_async_remote_copy(
            src_ref=src, dst_ref=dst, send_sem=send_sem.at[out_i], recv_sem=recv_sem.at[i],
            device_id=(partner[bit] if target is None else target,), device_id_type=MESH,
        )
        copy.start()
        sent.append((copy, out_i))
        return copy

    def reap(count):
        while len(sent) > count:
            copy, i = sent.pop(0)
            copy.wait_send()
            free.append(i)

    sent = []
    free = list(range(send_sem.shape[0]))
    upper = pl.ds(1, top)
    get_p = loads(p_hbm, p, 0)
    get_s0 = loads(s_hbm.at[0], s.at[0], 1)
    get_c0 = loads(c_hbm.at[0], cap.at[0], 2)
    get_x = loads(x_hbm, x, 3)
    get_i = loads(inv_hbm.at[0], inv, 4)
    get_s = loads(s_hbm.at[upper], s.at[upper], 5)
    get_c = loads(c_hbm.at[upper], cap.at[upper], 6)
    barrier = pltpu.get_barrier_semaphore()
    for b in range(levels):
        pl.semaphore_signal(barrier, inc=1, device_id=(partner[b],), device_id_type=MESH)
    pl.semaphore_signal(barrier, inc=1, device_id=(diagonal,), device_id_type=MESH)

    g_copy = {}
    k_copy = {}
    z_copy = {}
    c_copy = {}

    get_p.wait()
    for m in range(1, levels):
        p_t[m] = p[m].T
    get_s0.wait()
    products = dot_nn(p_t[1:levels].reshape(top * rank, seg), s[0]).astype(BF16)
    get_c0.wait()
    k0s[...] = dot_nn(products, cap[0]).astype(BF16)
    pl.semaphore_wait(barrier, levels + 1)
    k_copy[0] = send(k0s, k0r, 0)

    get_x.wait()
    x_t = x[...].T
    get_i.wait()
    st = dot_nt(x_t, inv[...]).astype(BF16)
    for m in range(levels):
        y = dot_nn(st, p[m]).reshape(2, half, rank)
        y16[m] = y.astype(BF16)
        if m > 0:
            y32[m] = y
    z_copy[0, 0] = send(y16.at[0], y0r, 0)
    z_copy[0, 1] = send(y16.at[pl.ds(1, top), 1 - core], zr0.at[pl.ds(1, top)], 0)

    get_s.wait()
    get_c.wait()
    for l in range(levels - 2, 0, -1):
        products = dot_nn(p_t[l + 1 : levels].reshape((top - l) * rank, seg), s[l])
        if l == 1:
            g1f[...] = products
            g1s[...] = products.astype(BF16)
            g1_copy = send(g1s, g1r, 0)
        else:
            products = products.reshape(top - l, 2, hr, rank)
            g32[first[l] : first[l] + top - l] = products
            gs[0, first[l] : first[l] + top - l] = products.astype(BF16)
            if l == 2:
                g_copy[0] = send(gs.at[0, :, 1 - core], gr.at[0], 0)

    def g_step(b):
        lo = first[b + 1]
        if lo >= len(pairs):
            return
        g_copy[b].wait_recv()
        nxt = first[b + 2]
        for i in range(len(pairs) - 1, lo - 1, -1):
            old = g32[i, core] if b == 0 else g32[i, 0]
            g = old + gr[b, i].astype(F32)
            g32[i, 0] = g
            if i >= nxt:
                gs[b + 1, i, 0] = g.astype(BF16)
        if nxt < len(pairs):
            rest = pl.ds(nxt, len(pairs) - nxt)
            g_copy[b + 1] = send(gs.at[b + 1, rest, 0], gr.at[b + 1, rest], b + 1)
        if b >= 1:
            n = top - (b + 1)
            for j in range(n):
                ks[b + 1, j] = dot_nn(g32[lo + j, 0].astype(BF16), cap[b + 1]).astype(BF16)
            k_copy[b + 1] = send(ks.at[b + 1, pl.ds(0, n)], kr.at[b + 1, pl.ds(0, n)], b + 1)

    def k_sum(l):
        n = top - l
        k_copy[l].wait_recv()
        for j in range(n):
            kfull[l, j, core] = (ks[l, j].astype(F32) + kr[l, j].astype(F32)).astype(BF16)
        mine = kfull.at[l, pl.ds(0, n), core]
        return send(mine, mine, 0)

    def stack(own, other, l):
        low = side[l] == 0
        return jnp.concatenate([jnp.where(low, own, other), jnp.where(low, other, own)], 1)

    k_copy[0].wait_recv()
    k0r[...] = (k0s[...].astype(F32) + k0r[...].astype(F32)).astype(BF16)
    z_copy[0, 0].wait_recv()
    stacked = stack(y16[0, core], y0r[core], 0)
    z_copy[0, 1].wait_recv()
    for m in range(1, levels):
        z = y32[m, core] + zr0[m].astype(F32) - dot_nt(stacked, k0r[(m - 1) * rank : m * rank])
        if m == 1:
            z1s[...] = z.astype(BF16)
            z_copy[1, 1] = send(z1s, z1r, 1)
        else:
            zb32[m] = z.reshape(2, quarter, rank)
    g_step(0)
    g1_copy.wait_recv()
    g1s_sum = (g1f[...] + g1r[...].astype(F32)).astype(BF16)
    g1f[...] = g1s_sum.astype(F32)
    out[...] = dot_nn(inv[...], x[...])
    stacked = stack(y16[0].reshape(rhs, rank), y0r[...].reshape(rhs, rank), 0)
    coef[0] = dot_nt(stacked, cap[0]).astype(BF16).reshape(2, 2, quarter, rank)
    out[...] -= dot_nt(s[0], coef[0].reshape(rhs, rank))

    reap(2)
    z_copy[1, 1].wait_recv()
    c_one = dot_nt(stack(z1s[...], z1r[...], 1), cap[1]).astype(BF16)
    coef[1, core] = c_one.reshape(2, quarter, rank)
    for m in range(2, levels):
        g = g1f[(m - 2) * rank : (m - 1) * rank].astype(BF16)
        z = zb32[m] - dot_nt(c_one, g).reshape(2, quarter, rank)
        zb32[m] = z
        zb16[m] = z.astype(BF16)
        z_copy[1, m] = send(zb16.at[m, 1 - xside], zbr.at[m], 1)
    c_copy[1] = send(coef.at[1, core], coef.at[1, core], 0)
    g_step(1)
    for m in range(2, levels):
        z_copy[1, m].wait_recv()
        z = zb32[m, xside] + zbr[m].astype(F32)
        z32[m] = z
        zs[2, m] = z.astype(BF16)
        z_copy[2, m] = send(zs.at[2, m], zr.at[2, m], 2)
    g_step(2)
    k_done = k_sum(2)
    c_copy[1].wait_recv()
    out[...] -= dot_nt(s[1], coef[1].reshape(rhs, rank))

    for l in range(2, levels):
        reap(top + 2)
        z_copy[l, l].wait_recv()
        stacked = stack(zs[l, l], zr[l, l], l)
        if l < top:
            k_done.wait_recv()
            for m in range(l + 1, levels):
                z_copy[l, m].wait_recv()
                z = z32[m] + zr[l, m].astype(F32) - dot_nt(stacked, kfull[l, m - l - 1].reshape(rank, 2 * rank))
                z32[m] = z
                zs[l + 1, m] = z.astype(BF16)
                z_copy[l + 1, m] = send(zs.at[l + 1, m], zr.at[l + 1, m], l + 1)
        coef[l, core, xside] = dot_nt(stacked, cap[l]).astype(BF16)
        mine = coef.at[l, core, xside]
        c_copy[l] = [send(mine, mine, 1, diagonal), send(mine, mine, 1), send(mine, mine, 0)]
        if l < top:
            if l + 1 < top:
                g_step(l + 1)
                k_done = k_sum(l + 1)
    for l in range(2, levels):
        for copy in c_copy[l]:
            copy.wait_recv()
        if l < top:
            out[...] -= dot_nt(s[l], coef[l].reshape(rhs, rank))
    reap(0)
    assert used[0] == recv_sem.shape[0]
    c_last = coef[top].reshape(rhs, rank)
    out[...] -= dot_nt(s[top], c_last)


def on_device(right_side, leaf_inverse, project_rows, spread_rows, capacity):
    levels, seg, rank = project_rows.shape
    rhs = right_side.shape[1]
    half = rhs // 2
    quarter = half // 2
    hr = rank // 2
    pairs = max(1, (levels - 2) * (levels - 3) // 2)
    top = levels - 1
    copies = 5 + levels + top * (top - 1) // 2 + 3 * (top - 1) + 3 * (top - 2)
    sends = 3 * levels + 4
    vmem = pltpu.VMEM
    return pl.pallas_call(
        kernel,
        name="hodlr_solve",
        out_shape=pltpu.VMEM((seg, rhs), F32),
        in_specs=[pl.BlockSpec(memory_space=pltpu.HBM)] * 5,
        out_specs=pl.BlockSpec(memory_space=pltpu.VMEM),
        scratch_shapes=[
            vmem((seg, rhs), BF16),
            vmem((seg, seg), BF16),
            vmem((levels, seg, rank), BF16),
            vmem((levels, seg, rank), BF16),
            vmem((levels, rank, 2 * rank), BF16),
            vmem((levels, rank, seg), BF16),
            vmem((levels, 2, half, rank), F32),
            vmem((levels, 2, half, rank), BF16),
            vmem((2, half, rank), BF16),
            vmem((levels, half, rank), BF16),
            vmem((half, rank), BF16),
            vmem((half, rank), BF16),
            vmem((levels, 2, quarter, rank), F32),
            vmem((levels, 2, quarter, rank), BF16),
            vmem((levels, quarter, rank), BF16),
            vmem((levels, quarter, rank), F32),
            vmem((levels, levels, quarter, rank), BF16),
            vmem((levels, levels, quarter, rank), BF16),
            vmem((levels, 2, 2, quarter, rank), BF16),
            vmem(((levels - 2) * rank, rank), F32),
            vmem(((levels - 2) * rank, rank), BF16),
            vmem(((levels - 2) * rank, rank), BF16),
            vmem(((levels - 1) * rank, 2 * rank), BF16),
            vmem(((levels - 1) * rank, 2 * rank), BF16),
            vmem((levels - 1, levels - 1, 2, hr, 2 * rank), BF16),
            vmem((levels - 1, levels - 1, hr, 2 * rank), BF16),
            vmem((levels - 1, levels - 1, hr, 2 * rank), BF16),
            vmem((pairs, 2, hr, rank), F32),
            vmem((levels - 1, pairs, 2, hr, rank), BF16),
            vmem((levels - 1, pairs, hr, rank), BF16),
            pltpu.SemaphoreType.DMA((7,)),
            pltpu.SemaphoreType.DMA((sends,)),
            pltpu.SemaphoreType.DMA((copies,)),
        ],
        compiler_params=pltpu.CompilerParams(
            collective_id=0, has_side_effects=True, vmem_limit_bytes=56 * 2**20
        ),
    )(right_side, leaf_inverse, project_rows, spread_rows, capacity)


def solution(mesh):
    return jax.shard_map(
        on_device,
        mesh=mesh,
        in_specs=(
            P("seq", None),
            P("seq", None, None),
            P(None, "seq", None),
            P(None, "seq", None),
            P(None, "seq", None),
        ),
        out_specs=P("seq", None),
        check_vma=False,
    )
```

```python
import functools

import jax
import jax.numpy as jnp
from jax import lax
from jax.experimental import pallas as pl
from jax.experimental.pallas import tpu as pltpu
from jax.sharding import PartitionSpec as P

MESH = pl.DeviceIdType.MESH
BF16 = jnp.bfloat16
F32 = jnp.float32


def dot_nt(left, right):
    return lax.dot_general(left, right, (((1,), (1,)), ((), ())), preferred_element_type=F32)


def dot_nn(left, right):
    return jnp.dot(left, right, preferred_element_type=F32)


def kernel(
    x_hbm, inv_hbm, p_hbm, s_hbm, c_hbm, out,
    x, inv, p, s, cap, p_t,
    y32, y16, y0r, zr0, z1s, z1r, zb32, zb16, zbr, z32, zs, zr, coef,
    g1f, g1s, g1r, k0s, k0r, kfull, ks, kr, g32, gs, gr,
    load_sem, send_sem, recv_sem,
):
    levels, seg, rank = p.shape
    half = y32.shape[2]
    quarter = half // 2
    rhs = 2 * half
    hr = rank // 2
    top = levels - 1
    me = lax.axis_index("seq")
    side = [lax.rem(lax.div(me, 1 << b), 2) for b in range(levels)]
    partner = [me + (1 - 2 * side[b]) * (1 << b) for b in range(levels)]
    core = side[0]
    xside = side[1]
    diagonal = partner[1] + partner[0] - me
    pairs = [(l, m) for l in range(2, levels) for m in range(l + 1, levels)]
    first = {l: min([i for i, q in enumerate(pairs) if q[0] >= l], default=len(pairs)) for l in range(levels + 1)}
    used = [0]

    def loads(src, dst, i):
        copy = pltpu.make_async_copy(src, dst, load_sem.at[i])
        copy.start()
        return copy

    def send(src, dst, bit, target=None):
        i = used[0]
        used[0] += 1
        out_i = free.pop(0)
        copy = pltpu.make_async_remote_copy(
            src_ref=src, dst_ref=dst, send_sem=send_sem.at[out_i], recv_sem=recv_sem.at[i],
            device_id=(partner[bit] if target is None else target,), device_id_type=MESH,
        )
        copy.start()
        sent.append((copy, out_i))
        return copy

    def reap(count):
        while len(sent) > count:
            copy, i = sent.pop(0)
            copy.wait_send()
            free.append(i)

    sent = []
    free = list(range(send_sem.shape[0]))
    upper = pl.ds(1, top)
    get_p = loads(p_hbm, p, 0)
    get_s0 = loads(s_hbm.at[0], s.at[0], 1)
    get_c0 = loads(c_hbm.at[0], cap.at[0], 2)
    get_x = loads(x_hbm, x, 3)
    get_i = loads(inv_hbm.at[0], inv, 4)
    get_s = loads(s_hbm.at[upper], s.at[upper], 5)
    get_c = loads(c_hbm.at[upper], cap.at[upper], 6)
    barrier = pltpu.get_barrier_semaphore()
    for b in range(levels):
        pl.semaphore_signal(barrier, inc=1, device_id=(partner[b],), device_id_type=MESH)
    pl.semaphore_signal(barrier, inc=1, device_id=(diagonal,), device_id_type=MESH)

    g_copy = {}
    k_copy = {}
    z_copy = {}
    c_copy = {}

    get_p.wait()
    for m in range(1, levels):
        p_t[m] = p[m].T
    get_s0.wait()
    products = dot_nn(p_t[1:levels].reshape(top * rank, seg), s[0]).astype(BF16)
    get_c0.wait()
    k0s[...] = dot_nn(products, cap[0]).astype(BF16)
    pl.semaphore_wait(barrier, levels + 1)
    k_copy[0] = send(k0s, k0r, 0)

    get_x.wait()
    x_t = x[...].T
    get_i.wait()
    st = dot_nt(x_t, inv[...]).astype(BF16)
    for m in range(levels):
        y = dot_nn(st, p[m]).reshape(2, half, rank)
        y16[m] = y.astype(BF16)
        if m > 0:
            y32[m] = y
    z_copy[0, 0] = send(y16.at[0], y0r, 0)
    z_copy[0, 1] = send(y16.at[pl.ds(1, top), 1 - core], zr0.at[pl.ds(1, top)], 0)

    get_s.wait()
    get_c.wait()
    for l in range(levels - 2, 0, -1):
        products = dot_nn(p_t[l + 1 : levels].reshape((top - l) * rank, seg), s[l])
        if l == 1:
            g1f[...] = products
            g1s[...] = products.astype(BF16)
            g1_copy = send(g1s, g1r, 0)
        else:
            products = products.reshape(top - l, 2, hr, rank)
            g32[first[l] : first[l] + top - l] = products
            gs[0, first[l] : first[l] + top - l] = products.astype(BF16)
            if l == 2:
                g_copy[0] = send(gs.at[0, :, 1 - core], gr.at[0], 0)

    def g_step(b):
        lo = first[b + 1]
        if lo >= len(pairs):
            return
        g_copy[b].wait_recv()
        nxt = first[b + 2]
        for i in range(len(pairs) - 1, lo - 1, -1):
            old = g32[i, core] if b == 0 else g32[i, 0]
            g = old + gr[b, i].astype(F32)
            g32[i, 0] = g
            if i >= nxt:
                gs[b + 1, i, 0] = g.astype(BF16)
        if nxt < len(pairs):
            rest = pl.ds(nxt, len(pairs) - nxt)
            g_copy[b + 1] = send(gs.at[b + 1, rest, 0], gr.at[b + 1, rest], b + 1)
        if b >= 1:
            n = top - (b + 1)
            for j in range(n):
                ks[b + 1, j] = dot_nn(g32[lo + j, 0].astype(BF16), cap[b + 1]).astype(BF16)
                k_copy[b + 1, j] = send(ks.at[b + 1, j], kr.at[b + 1, j], b + 1)

    def k_sum(l):
        done = []
        for j in range(top - l):
            k_copy[l, j].wait_recv()
            kfull[l, j, core] = (ks[l, j].astype(F32) + kr[l, j].astype(F32)).astype(BF16)
            mine = kfull.at[l, j, core]
            done.append(send(mine, mine, 0))
        return done

    def stack(own, other, l):
        low = side[l] == 0
        return jnp.concatenate([jnp.where(low, own, other), jnp.where(low, other, own)], 1)

    k_copy[0].wait_recv()
    k0r[...] = (k0s[...].astype(F32) + k0r[...].astype(F32)).astype(BF16)
    z_copy[0, 0].wait_recv()
    stacked = stack(y16[0, core], y0r[core], 0)
    z_copy[0, 1].wait_recv()
    for m in range(1, levels):
        z = y32[m, core] + zr0[m].astype(F32) - dot_nt(stacked, k0r[(m - 1) * rank : m * rank])
        if m == 1:
            z1s[...] = z.astype(BF16)
            z_copy[1, 1] = send(z1s, z1r, 1)
        else:
            zb32[m] = z.reshape(2, quarter, rank)
    g_step(0)
    g1_copy.wait_recv()
    g1s_sum = (g1f[...] + g1r[...].astype(F32)).astype(BF16)
    g1f[...] = g1s_sum.astype(F32)
    out[...] = dot_nn(inv[...], x[...])
    stacked = stack(y16[0].reshape(rhs, rank), y0r[...].reshape(rhs, rank), 0)
    coef[0] = dot_nt(stacked, cap[0]).astype(BF16).reshape(2, 2, quarter, rank)
    out[...] -= dot_nt(s[0], coef[0].reshape(rhs, rank))

    reap(2)
    z_copy[1, 1].wait_recv()
    c_one = dot_nt(stack(z1s[...], z1r[...], 1), cap[1]).astype(BF16)
    coef[1, core] = c_one.reshape(2, quarter, rank)
    for m in range(2, levels):
        g = g1f[(m - 2) * rank : (m - 1) * rank].astype(BF16)
        z = zb32[m] - dot_nt(c_one, g).reshape(2, quarter, rank)
        zb32[m] = z
        zb16[m] = z.astype(BF16)
        z_copy[1, m] = send(zb16.at[m, 1 - xside], zbr.at[m], 1)
    c_copy[1] = send(coef.at[1, core], coef.at[1, core], 0)
    g_step(1)
    for m in range(2, levels):
        z_copy[1, m].wait_recv()
        z = zb32[m, xside] + zbr[m].astype(F32)
        z32[m] = z
        zs[2, m] = z.astype(BF16)
        z_copy[2, m] = send(zs.at[2, m], zr.at[2, m], 2)
    g_step(2)
    k_done = k_sum(2)
    c_copy[1].wait_recv()
    out[...] -= dot_nt(s[1], coef[1].reshape(rhs, rank))

    for l in range(2, levels):
        reap(top + 2)
        z_copy[l, l].wait_recv()
        stacked = stack(zs[l, l], zr[l, l], l)
        if l < top:
            for m in range(l + 1, levels):
                z_copy[l, m].wait_recv()
                k_done[m - l - 1].wait_recv()
                z = z32[m] + zr[l, m].astype(F32) - dot_nt(stacked, kfull[l, m - l - 1].reshape(rank, 2 * rank))
                z32[m] = z
                zs[l + 1, m] = z.astype(BF16)
                z_copy[l + 1, m] = send(zs.at[l + 1, m], zr.at[l + 1, m], l + 1)
        coef[l, core, xside] = dot_nt(stacked, cap[l]).astype(BF16)
        mine = coef.at[l, core, xside]
        c_copy[l] = [send(mine, mine, 1, diagonal), send(mine, mine, 1), send(mine, mine, 0)]
        if l < top:
            if l + 1 < top:
                g_step(l + 1)
                k_done = k_sum(l + 1)
    for l in range(2, levels):
        for copy in c_copy[l]:
            copy.wait_recv()
        if l < top:
            out[...] -= dot_nt(s[l], coef[l].reshape(rhs, rank))
    reap(0)
    assert used[0] == recv_sem.shape[0]
    c_last = coef[top].reshape(rhs, rank)
    out[...] -= dot_nt(s[top], c_last)


def on_device(right_side, leaf_inverse, project_rows, spread_rows, capacity):
    levels, seg, rank = project_rows.shape
    rhs = right_side.shape[1]
    half = rhs // 2
    quarter = half // 2
    hr = rank // 2
    pairs = max(1, (levels - 2) * (levels - 3) // 2)
    top = levels - 1
    copies = 5 + levels + top * (top - 1) // 2 + 3 * (top - 1) + (top - 2) * top
    sends = 5 * levels
    vmem = pltpu.VMEM
    return pl.pallas_call(
        kernel,
        name="hodlr_solve",
        out_shape=pltpu.VMEM((seg, rhs), F32),
        in_specs=[pl.BlockSpec(memory_space=pltpu.HBM)] * 5,
        out_specs=pl.BlockSpec(memory_space=pltpu.VMEM),
        scratch_shapes=[
            vmem((seg, rhs), BF16),
            vmem((seg, seg), BF16),
            vmem((levels, seg, rank), BF16),
            vmem((levels, seg, rank), BF16),
            vmem((levels, rank, 2 * rank), BF16),
            vmem((levels, rank, seg), BF16),
            vmem((levels, 2, half, rank), F32),
            vmem((levels, 2, half, rank), BF16),
            vmem((2, half, rank), BF16),
            vmem((levels, half, rank), BF16),
            vmem((half, rank), BF16),
            vmem((half, rank), BF16),
            vmem((levels, 2, quarter, rank), F32),
            vmem((levels, 2, quarter, rank), BF16),
            vmem((levels, quarter, rank), BF16),
            vmem((levels, quarter, rank), F32),
            vmem((levels, levels, quarter, rank), BF16),
            vmem((levels, levels, quarter, rank), BF16),
            vmem((levels, 2, 2, quarter, rank), BF16),
            vmem(((levels - 2) * rank, rank), F32),
            vmem(((levels - 2) * rank, rank), BF16),
            vmem(((levels - 2) * rank, rank), BF16),
            vmem(((levels - 1) * rank, 2 * rank), BF16),
            vmem(((levels - 1) * rank, 2 * rank), BF16),
            vmem((levels - 1, levels - 1, 2, hr, 2 * rank), BF16),
            vmem((levels - 1, levels - 1, hr, 2 * rank), BF16),
            vmem((levels - 1, levels - 1, hr, 2 * rank), BF16),
            vmem((pairs, 2, hr, rank), F32),
            vmem((levels - 1, pairs, 2, hr, rank), BF16),
            vmem((levels - 1, pairs, hr, rank), BF16),
            pltpu.SemaphoreType.DMA((7,)),
            pltpu.SemaphoreType.DMA((sends,)),
            pltpu.SemaphoreType.DMA((copies,)),
        ],
        compiler_params=pltpu.CompilerParams(
            collective_id=0, has_side_effects=True, vmem_limit_bytes=56 * 2**20
        ),
    )(right_side, leaf_inverse, project_rows, spread_rows, capacity)


def solution(mesh):
    return jax.shard_map(
        on_device,
        mesh=mesh,
        in_specs=(
            P("seq", None),
            P("seq", None, None),
            P(None, "seq", None),
            P(None, "seq", None),
            P(None, "seq", None),
        ),
        out_specs=P("seq", None),
        check_vma=False,
    )
```
